32 devices in a mesh: prow: 4 (over x, core), pcol: 8 (over z, y).
Axes of the slice: x: 2, y: 2, z: 4, core: 2. Of those that a mesh axis runs over, the one named last changes fastest.
Arguments:
- slab: float32 [16384, 2048], P('prow', 'pcol'), may hold values from -6 to 6
- panel: float32 [16384, 512], P(('prow', 'pcol')), may hold values from -0.25 to 0.25
- pivots: int32 [512], replicated, may hold values from 0 to 16383, as said below
- inv_lower: float32 [512, 512], replicated, as said below
- inv_upper: float32 [512, 512], replicated, as said below
Outputs:
- updated: float32 [16384, 2048], P('prow', 'pcol')
The draws below stay inside these ranges and needn't reach their ends.
Inputs may be any that keep to these rules, and one draw needn't show every extreme that they name: `pivots`: 512 distinct row indices. `inv_lower`: unit lower triangular. `inv_upper`: upper triangular with a positive diagonal.
All inputs are finite; a program needn't handle non-finite values.
Results may differ from the reference program's by a relative error of at most 0.000061.
Values sent between devices are 32-bit elements; how exact they have to be, the bound alone decides.
A program may use at most 64 MiB of HBM per device.

```python
import jax
import jax.numpy as jnp
from jax import lax

NB = 512
ROWS_DEV = 4096
NS_DEV = 256
M = 16384
NS = 2048
N_PROW = 4
N_PCOL = 8


def draw_pivots(key, part):
    order = jax.random.permutation(jax.random.fold_in(key, 11), ROWS_DEV * N_PROW)
    return order[:NB].astype(jnp.int32)


def draw_inv_lower(key, part):
    sub_key = jax.random.fold_in(key, 23)
    entries = jax.random.normal(sub_key, (NB, NB), jnp.float32)
    return jnp.tril(entries, -1) * NB ** (-0.5) + jnp.eye(NB, dtype=jnp.float32)


def draw_inv_upper(key, part):
    sub_key = jax.random.fold_in(key, 37)
    diag_key = jax.random.fold_in(key, 41)
    entries = jax.random.normal(sub_key, (NB, NB), jnp.float32)
    diagonal = jax.random.uniform(diag_key, (NB,), jnp.float32, 0.5, 1.5)
    return jnp.triu(entries, 1) * NB ** (-0.5) + jnp.diag(diagonal)


def shard_levels(key, extent, split, least, high):
    def one(dim, parts):
        steps = jax.random.uniform(jax.random.fold_in(jax.random.fold_in(key, 6), dim), (parts,), jnp.float32, least / len(split), high / len(split))
        return jnp.repeat(jnp.exp(steps), extent[dim] // parts).reshape((-1,) + (1,) * (len(extent) - dim - 1))

    gain = one(*split[0])
    for cut in split[1:]:
        gain = gain * one(*cut)
    return gain


def normal_values(rng, shape, scale, bound, split=(), kind=jnp.bfloat16):
    values = scale * jax.random.normal(rng, shape, jnp.float32)
    if split:
        values = values * shard_levels(rng, shape, split, -0.22, 0.18)
    return jnp.clip(values, -bound, bound).astype(kind)


def setup_inputs(seed: int = 0) -> dict:
    arg_keys = jax.random.split(jax.random.key(seed), 6)
    return {
        "slab": normal_values(arg_keys[0], (M, NS), 1.0, 6.0, ((0, 4), (1, 8)), jnp.float32),
        "panel": normal_values(arg_keys[1], (M, NB), NB ** -0.5, 0.25, ((0, 32),), jnp.float32),
        "pivots": draw_pivots(jax.random.fold_in(arg_keys[5], 71), 0),
        "inv_lower": draw_inv_lower(jax.random.fold_in(arg_keys[5], 71), 0),
        "inv_upper": draw_inv_upper(jax.random.fold_in(arg_keys[5], 71), 0),
    }


def reference(slab, panel, pivots, inv_lower, inv_upper):
    pivot_rows = jnp.take(slab, pivots.astype(jnp.int32), axis=0)
    upper_block = jnp.dot(inv_lower, pivot_rows, precision=lax.Precision.HIGHEST, preferred_element_type=jnp.float32)
    panel_blocks = panel.reshape(N_PROW, ROWS_DEV, NB)
    slab_blocks = slab.reshape(N_PROW, ROWS_DEV, NS_DEV * N_PCOL)

    def one_block(operands):
        panel_block, slab_block = operands
        lower_rows = jnp.dot(panel_block, inv_upper, precision=lax.Precision.HIGHEST, preferred_element_type=jnp.float32)
        product = jnp.dot(lower_rows, upper_block, precision=lax.Precision.HIGHEST, preferred_element_type=jnp.float32)
        return slab_block - product

    updated = lax.map(one_block, (panel_blocks, slab_blocks)).reshape(slab.shape)
    updated = updated.at[pivots.astype(jnp.int32)].set(upper_block)
    return updated
```

```python
import functools

import jax
import jax.numpy as jnp
from jax import lax
from jax.experimental import pallas as pl
from jax.experimental.pallas import tpu as pltpu
from jax.sharding import PartitionSpec as P

MESH = pl.DeviceIdType.MESH
HIGHEST = lax.Precision.HIGHEST
F32 = jnp.float32


def dot(a, b):
    return jnp.dot(a, b, precision=HIGHEST, preferred_element_type=F32)


def kernel(
    n_x, n_z, parts,
    slab_ref, panel_ref, pivots_ref, pivot_row_ref, inv_lower_ref, inv_upper_ref,
    out_ref,
    slab, raw, lower, stage, landed, inv_lower, inv_upper,
    picked, partner_part, chip_sum, from_x, total, halves, upper, upper_peer,
    load_sem, link_send, link_recv, product_send, product_recv, out_sem,
    pick_send, pick_recv, x_send, x_recv, half_send, half_recv,
):
    prow = lax.axis_index("prow")
    pcol = lax.axis_index("pcol")
    x, core = prow // 2, prow % 2
    z, y = pcol // 2, pcol % 2
    rows = panel_ref.shape[0]
    nb = panel_ref.shape[1]
    piece = rows // parts
    row_count, columns = slab_ref.shape
    half = columns // 2
    first_row = prow * row_count
    partner = {"prow": x * 2 + 1 - core}
    peer = {"pcol": z * 2 + 1 - y}
    left = {"pcol": (z - 1) * 2 + y}
    right = {"pcol": (z + 1) * 2 + y}
    has_left, has_right = z > 0, z < n_z - 1

    loads = [
        pltpu.make_async_copy(slab_ref, slab, load_sem.at[0]),
        pltpu.make_async_copy(panel_ref, raw.at[z], load_sem.at[1]),
        pltpu.make_async_copy(inv_upper_ref, inv_upper, load_sem.at[2]),
        pltpu.make_async_copy(inv_lower_ref, inv_lower, load_sem.at[3]),
    ]
    for load in loads:
        load.start()

    barrier = pltpu.get_barrier_semaphore()
    fixed = [partner, peer] + [
        {"prow": lax.rem(x + o, n_x) * 2 + core} for o in range(1, n_x)
    ]
    for device in fixed:
        pl.semaphore_signal(barrier, inc=1, device_id=device, device_id_type=MESH)
    for exists, device in ((has_left, left), (has_right, right)):
        @pl.when(exists)
        def _():
            pl.semaphore_signal(barrier, inc=1, device_id=device, device_id_type=MESH)
    n_peers = len(fixed) + has_left.astype(jnp.int32) + has_right.astype(jnp.int32)
    pl.semaphore_wait(barrier, n_peers)

    def slot(direction, step, g):
        return (direction * (n_z - 1) + step) * parts + g

    def send(direction, step, g):
        block = z - step if direction == 0 else z + step
        span = pl.ds(g * piece, piece)
        source = panel_ref.at[span] if isinstance(step, int) else raw.at[block, span]
        return pltpu.make_async_remote_copy(
            src_ref=source,
            dst_ref=raw.at[block, span],
            send_sem=link_send.at[slot(direction, step, g)],
            recv_sem=link_recv.at[slot(direction, step, g)],
            device_id=right if direction == 0 else left,
            device_id_type=MESH,
        )

    def sends(direction, step):
        if direction == 0:
            return has_right & (z - step >= 0)
        return has_left & (z + step < n_z)

    def receives(direction, step):
        if direction == 0:
            return z - 1 - step >= 0
        return z + 1 + step < n_z

    def arrived(direction, step, g):
        block = z - 1 - step if direction == 0 else z + 1 + step
        span = pl.ds(g * piece, piece)
        pltpu.make_async_remote_copy(
            src_ref=raw.at[block, span],
            dst_ref=raw.at[block, span],
            send_sem=link_send.at[slot(direction, step, g)],
            recv_sem=link_recv.at[slot(direction, step, g)],
            device_id=left if direction == 0 else right,
            device_id_type=MESH,
        ).wait_recv()
        return block

    for g in range(parts):
        for direction in (0, 1):
            @pl.when(sends(direction, 0))
            def _():
                send(direction, 0, g).start()

    loads[0].wait()

    def pick(k, carry):
        local = pivots_ref[k] - first_row
        inside = (local >= 0) & (local < row_count)
        row = slab[pl.ds(jnp.where(inside, local, 0), 1), :]
        row = jnp.where(inside, row, 0.0)
        picked[0, pl.ds(k, 1), :] = row[:, :half]
        picked[1, pl.ds(k, 1), :] = row[:, half:]
        return carry

    lax.fori_loop(0, nb, pick, 0, unroll=8)

    def remote(source, target, send_sem, recv_sem, device):
        return pltpu.make_async_remote_copy(
            src_ref=source, dst_ref=target, send_sem=send_sem, recv_sem=recv_sem,
            device_id=device, device_id_type=MESH,
        )

    pick_copy = remote(picked.at[1 - core], partner_part, pick_send, pick_recv, partner)
    pick_copy.start()

    def pivot_hits(block, side, g):
        row = first_row + (block * 2 + side) * rows + g * piece
        ids = row + lax.broadcasted_iota(jnp.int32, (piece, nb), 0)
        hits = jnp.where(ids == pivot_row_ref[...], 1.0, 0.0)
        return hits, jnp.max(hits, axis=1, keepdims=True) > 0.0

    def make_lower(block, g):
        span = pl.ds(g * piece, piece)
        solved = dot(raw[block, span, :], inv_upper[...])
        hits, is_pivot = pivot_hits(block, y, g)
        lower[block, span, :] = jnp.where(is_pivot, -hits, solved)

    pick_copy.wait()
    chip_sum[...] = picked[core] + partner_part[...]
    x_copies = []
    for o in range(1, n_x):
        device = {"prow": lax.rem(x + o, n_x) * 2 + core}
        copy = remote(chip_sum, from_x.at[o - 1], x_send.at[o - 1], x_recv.at[o - 1], device)
        copy.start()
        x_copies.append(copy)

    loads[1].wait()
    loads[2].wait()
    loads[3].wait()
    lax.fori_loop(0, parts, lambda g, c: (make_lower(z, g), c)[1], 0)

    for copy in x_copies:
        copy.wait()
    summed = chip_sum[...]
    for o in range(1, n_x):
        summed = summed + from_x[o - 1]
    total[...] = summed
    halves[core] = dot(inv_lower[...], total[...])
    to_peer = remote(
        halves.at[core], halves.at[2 + core], half_send.at[0], half_recv.at[0], peer
    )
    to_partner = remote(
        halves.at[core], halves.at[core], half_send.at[1], half_recv.at[1], partner
    )
    to_peer.start()
    to_partner.start()

    def pass_on(step, g):
        for direction in (0, 1):
            @pl.when(receives(direction, step))
            def _():
                arrived(direction, step, g)

            @pl.when(receives(direction, step) & sends(direction, step + 1))
            def _():
                send(direction, step + 1, g).start()

    def blocks_of(stage_index):
        step = stage_index - 1
        return (
            (receives(0, step), z - 1 - step),
            (receives(1, step), z + 1 + step),
        )

    def first_stage(g, carry):
        pass_on(jnp.int32(0), g)
        for exists, block in blocks_of(1):
            @pl.when(exists)
            def _():
                make_lower(block, g)
        return carry

    lax.fori_loop(0, parts, first_stage, 0)

    to_partner.wait()
    to_peer.wait()
    onward = remote(
        halves.at[2 + core], halves.at[2 + core], half_send.at[2], half_recv.at[2], partner
    )
    onward.start()
    upper[:, :half] = halves[0]
    upper[:, half:] = halves[1]
    onward.wait()
    upper_peer[:, :half] = halves[2]
    upper_peer[:, half:] = halves[3]

    def product_copy(block, g):
        span = pl.ds(g * piece, piece)
        index = block * parts + g
        return remote(
            stage.at[block, span], landed.at[block, span],
            product_send.at[index], product_recv.at[index], peer,
        )

    def out_copy(block, side, g):
        start = (block * 2 + side) * rows + g * piece
        span = pl.ds(pl.multiple_of(start, 8), piece)
        index = (block * 2 + side) * parts + g
        return pltpu.make_async_copy(slab.at[span], out_ref.at[span], out_sem.at[index])

    def finish(block, side, g, product, is_pivot):
        start = (block * 2 + side) * rows + g * piece
        span = pl.ds(pl.multiple_of(start, 8), piece)
        slab[span, :] = jnp.where(is_pivot, 0.0, slab[span, :]) - product
        out_copy(block, side, g).start()

    def multiply(block, g):
        span = pl.ds(g * piece, piece)
        stage[block, span, :] = dot(lower[block, span, :], upper_peer[...])
        product_copy(block, g).start()
        _, is_pivot = pivot_hits(block, y, g)
        finish(block, y, g, dot(lower[block, span, :], upper[...]), is_pivot)

    def take(block, g):
        product_copy(block, g).wait_recv()
        _, is_pivot = pivot_hits(block, 1 - y, g)
        span = pl.ds(g * piece, piece)
        finish(block, 1 - y, g, landed[block, span, :], is_pivot)

    lax.fori_loop(0, parts, lambda g, c: (multiply(z, g), c)[1], 0)

    def second_stage(g, carry):
        for exists, block in blocks_of(1):
            @pl.when(exists)
            def _():
                multiply(block, g)
        return carry

    lax.fori_loop(0, parts, second_stage, 0)

    def late_stage(i, carry):
        stage_index, g = 2 + i // parts, i % parts
        pass_on(stage_index - 1, g)
        for exists, block in blocks_of(stage_index):
            @pl.when(exists)
            def _():
                make_lower(block, g)
                multiply(block, g)

        @pl.when(stage_index == 2)
        def _():
            take(z, g)

        for exists, block in blocks_of(stage_index - 2):
            @pl.when(exists & (stage_index > 2))
            def _():
                take(block, g)
        return carry

    lax.fori_loop(0, (n_z - 2) * parts, late_stage, 0)

    def last_stage(i, carry):
        stage_index, g = n_z - 2 + i // parts, i % parts

        if n_z == 2:
            @pl.when(stage_index == 0)
            def _():
                take(z, g)

        for exists, block in blocks_of(stage_index):
            @pl.when(exists & (stage_index > 0))
            def _():
                take(block, g)
        return carry

    lax.fori_loop(0, 2 * parts, last_stage, 0)

    def settle(i, carry):
        block, g = i // parts, i % parts
        product_copy(block, g).wait_send()
        out_copy(block, 0, g).wait()
        out_copy(block, 1, g).wait()
        return carry

    lax.fori_loop(0, n_z * parts, settle, 0)

    def settle_links(i, carry):
        step, g = i // parts, i % parts
        for direction in (0, 1):
            @pl.when(sends(direction, step))
            def _():
                send(direction, step, g).wait_send()
        return carry

    lax.fori_loop(0, (n_z - 1) * parts, settle_links, 0)


def solution(mesh):
    n_prow, n_pcol = mesh.shape["prow"], mesh.shape["pcol"]
    n_x, n_z, parts = n_prow // 2, n_pcol // 2, 4

    def local(slab, panel, pivots, inv_lower, inv_upper):
        (row_count, columns), (rows, nb) = slab.shape, panel.shape
        half = columns // 2
        links = 2 * (n_z - 1) * parts
        any_space = pl.BlockSpec(memory_space=pl.ANY)
        dma = pltpu.SemaphoreType.DMA
        flops = 2 * row_count * nb * (nb + columns)
        return pl.pallas_call(
            functools.partial(kernel, n_x, n_z, parts),
            out_shape=jax.ShapeDtypeStruct(slab.shape, slab.dtype),
            in_specs=[
                any_space,
                any_space,
                pl.BlockSpec(memory_space=pltpu.SMEM),
                pl.BlockSpec(memory_space=pltpu.VMEM),
                any_space,
                any_space,
            ],
            out_specs=any_space,
            scratch_shapes=[
                pltpu.VMEM((row_count, columns), F32),
                pltpu.VMEM((n_z, rows, nb), F32),
                pltpu.VMEM((n_z, rows, nb), F32),
                pltpu.VMEM((n_z, rows, columns), F32),
                pltpu.VMEM((n_z, rows, columns), F32),
                pltpu.VMEM((nb, nb), F32),
                pltpu.VMEM((nb, nb), F32),
                pltpu.VMEM((2, nb, half), F32),
                pltpu.VMEM((nb, half), F32),
                pltpu.VMEM((nb, half), F32),
                pltpu.VMEM((max(n_x - 1, 1), nb, half), F32),
                pltpu.VMEM((nb, half), F32),
                pltpu.VMEM((4, nb, half), F32),
                pltpu.VMEM((nb, columns), F32),
                pltpu.VMEM((nb, columns), F32),
                dma((4,)),
                dma((links,)),
                dma((links,)),
                dma((n_z * parts,)),
                dma((n_z * parts,)),
                dma((2 * n_z * parts,)),
                dma,
                dma,
                dma((max(n_x - 1, 1),)),
                dma((max(n_x - 1, 1),)),
                dma((3,)),
                dma((3,)),
            ],
            compiler_params=pltpu.CompilerParams(
                collective_id=0, has_side_effects=True, vmem_limit_bytes=60 * 2**20
            ),
            cost_estimate=pl.CostEstimate(
                flops=flops, bytes_accessed=8 * slab.size, transcendentals=0
            ),
        )(slab, panel, pivots, pivots.reshape(1, nb), inv_lower, inv_upper)

    return jax.shard_map(
        local,
        mesh=mesh,
        in_specs=(P("prow", "pcol"), P(("prow", "pcol"), None), P(), P(), P()),
        out_specs=P("prow", "pcol"),
        check_vma=False,
    )
```

```python
import functools

import jax
import jax.numpy as jnp
from jax import lax
from jax.experimental import pallas as pl
from jax.experimental.pallas import tpu as pltpu
from jax.sharding import PartitionSpec as P

MESH = pl.DeviceIdType.MESH
HIGHEST = lax.Precision.HIGHEST
F32 = jnp.float32
BF16 = jnp.bfloat16


def dot(a, b):
    return jnp.dot(a, b, precision=HIGHEST, preferred_element_type=F32)


def split(a):
    high = a.astype(BF16)
    return high, (a - high.astype(F32)).astype(BF16)


def dot_split(a_high, a_low, b_high, b_low):
    rows = a_high.shape[0]
    both = jnp.dot(
        jnp.concatenate([a_high, a_low], axis=0), b_high, preferred_element_type=F32
    )
    cross = jnp.dot(a_high, b_low, preferred_element_type=F32)
    return both[:rows] + (both[rows:] + cross)


def kernel(
    n_x, n_z, parts,
    slab_ref, panel_ref, pivots_ref, pivot_row_ref, inv_lower_ref, inv_upper_ref,
    out_ref,
    raw, lower, stage, landed, inv_lower, inv_upper, inv_split,
    picked, partner_part, chip_sum, from_x, total, halves, upper,
    load_sem, link_send, link_recv, product_send, product_recv,
    pick_send, pick_recv, x_send, x_recv, half_send, half_recv,
):
    slab = out_ref
    prow = lax.axis_index("prow")
    pcol = lax.axis_index("pcol")
    x, core = prow // 2, prow % 2
    z, y = pcol // 2, pcol % 2
    rows = panel_ref.shape[0]
    nb = panel_ref.shape[1]
    piece = rows // parts
    row_count, columns = slab_ref.shape
    half = columns // 2
    first_row = prow * row_count
    partner = {"prow": x * 2 + 1 - core}
    peer = {"pcol": z * 2 + 1 - y}
    left = {"pcol": (z - 1) * 2 + y}
    right = {"pcol": (z + 1) * 2 + y}
    has_left, has_right = z > 0, z < n_z - 1

    loads = [
        pltpu.make_async_copy(slab_ref, slab, load_sem.at[0]),
        pltpu.make_async_copy(panel_ref, raw.at[z], load_sem.at[1]),
        pltpu.make_async_copy(inv_upper_ref, inv_upper, load_sem.at[2]),
        pltpu.make_async_copy(inv_lower_ref, inv_lower, load_sem.at[3]),
    ]
    for load in loads:
        load.start()

    barrier = pltpu.get_barrier_semaphore()
    fixed = [partner, peer] + [
        {"prow": lax.rem(x + o, n_x) * 2 + core} for o in range(1, n_x)
    ]
    for device in fixed:
        pl.semaphore_signal(barrier, inc=1, device_id=device, device_id_type=MESH)
    for exists, device in ((has_left, left), (has_right, right)):
        @pl.when(exists)
        def _():
            pl.semaphore_signal(barrier, inc=1, device_id=device, device_id_type=MESH)
    n_peers = len(fixed) + has_left.astype(jnp.int32) + has_right.astype(jnp.int32)
    pl.semaphore_wait(barrier, n_peers)

    def slot(direction, step, g):
        return (direction * (n_z - 1) + step) * parts + g

    def send(direction, step, g):
        block = z - step if direction == 0 else z + step
        span = pl.ds(g * piece, piece)
        source = panel_ref.at[span] if isinstance(step, int) else raw.at[block, span]
        return pltpu.make_async_remote_copy(
            src_ref=source,
            dst_ref=raw.at[block, span],
            send_sem=link_send.at[slot(direction, step, g)],
            recv_sem=link_recv.at[slot(direction, step, g)],
            device_id=right if direction == 0 else left,
            device_id_type=MESH,
        )

    def sends(direction, step):
        if direction == 0:
            return has_right & (z - step >= 0)
        return has_left & (z + step < n_z)

    def receives(direction, step):
        if direction == 0:
            return z - 1 - step >= 0
        return z + 1 + step < n_z

    def arrived(direction, step, g):
        block = z - 1 - step if direction == 0 else z + 1 + step
        span = pl.ds(g * piece, piece)
        pltpu.make_async_remote_copy(
            src_ref=raw.at[block, span],
            dst_ref=raw.at[block, span],
            send_sem=link_send.at[slot(direction, step, g)],
            recv_sem=link_recv.at[slot(direction, step, g)],
            device_id=left if direction == 0 else right,
            device_id_type=MESH,
        ).wait_recv()
        return block

    for g in range(parts):
        for direction in (0, 1):
            @pl.when(sends(direction, 0))
            def _():
                send(direction, 0, g).start()

    loads[0].wait()

    def pick(k, carry):
        local = pivots_ref[k] - first_row
        inside = (local >= 0) & (local < row_count)
        row = slab[pl.ds(jnp.where(inside, local, 0), 1), :]
        row = jnp.where(inside, row, 0.0)
        picked[0, pl.ds(k, 1), :] = row[:, :half]
        picked[1, pl.ds(k, 1), :] = row[:, half:]
        return carry

    lax.fori_loop(0, nb, pick, 0, unroll=8)

    def remote(source, target, send_sem, recv_sem, device):
        return pltpu.make_async_remote_copy(
            src_ref=source, dst_ref=target, send_sem=send_sem, recv_sem=recv_sem,
            device_id=device, device_id_type=MESH,
        )

    pick_copy = remote(picked.at[1 - core], partner_part, pick_send, pick_recv, partner)
    pick_copy.start()

    def pivot_hits(block, side, g):
        row = first_row + (block * 2 + side) * rows + g * piece
        ids = row + lax.broadcasted_iota(jnp.int32, (piece, nb), 0)
        hits = jnp.where(ids == pivot_row_ref[...], 1.0, 0.0)
        return hits, jnp.max(hits, axis=1, keepdims=True) > 0.0

    def make_lower(block, g):
        span = pl.ds(g * piece, piece)
        high, low = split(raw[block, span, :])
        solved = dot_split(high, low, inv_split[0], inv_split[1])
        hits, is_pivot = pivot_hits(block, y, g)
        high, low = split(jnp.where(is_pivot, -hits, solved))
        lower[0, block, span, :] = high
        lower[1, block, span, :] = low

    pick_copy.wait()
    chip_sum[...] = picked[core] + partner_part[...]
    x_copies = []
    for o in range(1, n_x):
        device = {"prow": lax.rem(x + o, n_x) * 2 + core}
        copy = remote(chip_sum, from_x.at[o - 1], x_send.at[o - 1], x_recv.at[o - 1], device)
        copy.start()
        x_copies.append(copy)

    loads[1].wait()
    loads[2].wait()
    loads[3].wait()
    inv_split[0], inv_split[1] = split(inv_upper[...])
    lax.fori_loop(0, parts, lambda g, c: (make_lower(z, g), c)[1], 0)

    for copy in x_copies:
        copy.wait()
    summed = chip_sum[...]
    for o in range(1, n_x):
        summed = summed + from_x[o - 1]
    total[...] = summed
    halves[core] = dot(inv_lower[...], total[...])
    to_peer = remote(
        halves.at[core], halves.at[2 + core], half_send.at[0], half_recv.at[0], peer
    )
    to_partner = remote(
        halves.at[core], halves.at[core], half_send.at[1], half_recv.at[1], partner
    )
    to_peer.start()
    to_partner.start()

    def pass_on(step, g):
        for direction in (0, 1):
            @pl.when(receives(direction, step))
            def _():
                arrived(direction, step, g)

            @pl.when(receives(direction, step) & sends(direction, step + 1))
            def _():
                send(direction, step + 1, g).start()

    def blocks_of(stage_index):
        step = stage_index - 1
        return (
            (receives(0, step), z - 1 - step),
            (receives(1, step), z + 1 + step),
        )

    def first_stage(g, carry):
        pass_on(jnp.int32(0), g)
        for exists, block in blocks_of(1):
            @pl.when(exists)
            def _():
                make_lower(block, g)
        return carry

    lax.fori_loop(0, parts, first_stage, 0)

    to_partner.wait()
    to_peer.wait()
    onward = remote(
        halves.at[2 + core], halves.at[2 + core], half_send.at[2], half_recv.at[2], partner
    )
    onward.start()
    for i in (0, 1):
        upper[0, :, i * half:(i + 1) * half], upper[1, :, i * half:(i + 1) * half] = (
            split(halves[i])
        )
    onward.wait()
    for i in (2, 3):
        upper[0, :, i * half:(i + 1) * half], upper[1, :, i * half:(i + 1) * half] = (
            split(halves[i])
        )

    def product_copy(block, g):
        span = pl.ds(g * piece, piece)
        index = block * parts + g
        return remote(
            stage.at[block, span], landed.at[block, span],
            product_send.at[index], product_recv.at[index], peer,
        )

    def finish(block, side, g, product, is_pivot):
        start = (block * 2 + side) * rows + g * piece
        span = pl.ds(pl.multiple_of(start, 8), piece)
        slab[span, :] = jnp.where(is_pivot, 0.0, slab[span, :]) - product

    def multiply(block, g):
        span = pl.ds(g * piece, piece)
        products = dot_split(
            lower[0, block, span, :], lower[1, block, span, :], upper[0], upper[1]
        )
        stage[block, span, :] = products[:, columns:]
        product_copy(block, g).start()
        _, is_pivot = pivot_hits(block, y, g)
        finish(block, y, g, products[:, :columns], is_pivot)

    def take(block, g):
        product_copy(block, g).wait_recv()
        _, is_pivot = pivot_hits(block, 1 - y, g)
        span = pl.ds(g * piece, piece)
        finish(block, 1 - y, g, landed[block, span, :], is_pivot)

    lax.fori_loop(0, parts, lambda g, c: (multiply(z, g), c)[1], 0)

    def second_stage(g, carry):
        for exists, block in blocks_of(1):
            @pl.when(exists)
            def _():
                multiply(block, g)
        return carry

    lax.fori_loop(0, parts, second_stage, 0)

    def late_stage(i, carry):
        stage_index, g = 2 + i // parts, i % parts
        pass_on(stage_index - 1, g)
        for exists, block in blocks_of(stage_index):
            @pl.when(exists)
            def _():
                make_lower(block, g)
                multiply(block, g)

        @pl.when(stage_index == 2)
        def _():
            take(z, g)

        for exists, block in blocks_of(stage_index - 2):
            @pl.when(exists & (stage_index > 2))
            def _():
                take(block, g)
        return carry

    lax.fori_loop(0, (n_z - 2) * parts, late_stage, 0)

    def last_stage(i, carry):
        stage_index, g = n_z - 2 + i // parts, i % parts

        if n_z == 2:
            @pl.when(stage_index == 0)
            def _():
                take(z, g)

        for exists, block in blocks_of(stage_index):
            @pl.when(exists & (stage_index > 0))
            def _():
                take(block, g)
        return carry

    lax.fori_loop(0, 2 * parts, last_stage, 0)

    def settle(i, carry):
        block, g = i // parts, i % parts
        product_copy(block, g).wait_send()
        return carry

    lax.fori_loop(0, n_z * parts, settle, 0)

    def settle_links(i, carry):
        step, g = i // parts, i % parts
        for direction in (0, 1):
            @pl.when(sends(direction, step))
            def _():
                send(direction, step, g).wait_send()
        return carry

    lax.fori_loop(0, (n_z - 1) * parts, settle_links, 0)


def solution(mesh):
    n_prow, n_pcol = mesh.shape["prow"], mesh.shape["pcol"]
    n_x, n_z, parts = n_prow // 2, n_pcol // 2, 4

    def local(slab, panel, pivots, inv_lower, inv_upper):
        (row_count, columns), (rows, nb) = slab.shape, panel.shape
        half = columns // 2
        links = 2 * (n_z - 1) * parts
        hbm = pl.BlockSpec(memory_space=pltpu.HBM)
        dma = pltpu.SemaphoreType.DMA
        flops = 2 * row_count * nb * (nb + columns)
        return pl.pallas_call(
            functools.partial(kernel, n_x, n_z, parts),
            out_shape=pltpu.VMEM(slab.shape, slab.dtype),
            in_specs=[
                hbm,
                hbm,
                pl.BlockSpec(memory_space=pltpu.SMEM),
                pl.BlockSpec(memory_space=pltpu.VMEM),
                hbm,
                hbm,
            ],
            out_specs=pl.BlockSpec(memory_space=pltpu.VMEM),
            scratch_shapes=[
                pltpu.VMEM((n_z, rows, nb), F32),
                pltpu.VMEM((2, n_z, rows, nb), BF16),
                pltpu.VMEM((n_z, rows, columns), F32),
                pltpu.VMEM((n_z, rows, columns), F32),
                pltpu.VMEM((nb, nb), F32),
                pltpu.VMEM((nb, nb), F32),
                pltpu.VMEM((2, nb, nb), BF16),
                pltpu.VMEM((2, nb, half), F32),
                pltpu.VMEM((nb, half), F32),
                pltpu.VMEM((nb, half), F32),
                pltpu.VMEM((max(n_x - 1, 1), nb, half), F32),
                pltpu.VMEM((nb, half), F32),
                pltpu.VMEM((4, nb, half), F32),
                pltpu.VMEM((2, nb, 2 * columns), BF16),
                dma((4,)),
                dma((links,)),
                dma((links,)),
                dma((n_z * parts,)),
                dma((n_z * parts,)),
                dma,
                dma,
                dma((max(n_x - 1, 1),)),
                dma((max(n_x - 1, 1),)),
                dma((3,)),
                dma((3,)),
            ],
            compiler_params=pltpu.CompilerParams(
                collective_id=0, has_side_effects=True, vmem_limit_bytes=32 * 2**20
            ),
            cost_estimate=pl.CostEstimate(
                flops=flops, bytes_accessed=8 * slab.size, transcendentals=0
            ),
        )(
            *(pltpu.with_memory_space_constraint(a, pltpu.HBM) for a in (slab, panel)),
            pivots,
            pivots.reshape(1, nb),
            *(pltpu.with_memory_space_constraint(a, pltpu.HBM) for a in (inv_lower, inv_upper)),
        )

    return jax.shard_map(
        local,
        mesh=mesh,
        in_specs=(P("prow", "pcol"), P(("prow", "pcol"), None), P(), P(), P()),
        out_specs=P("prow", "pcol"),
        check_vma=False,
    )
```

```python
import functools

import jax
import jax.numpy as jnp
from jax import lax
from jax.experimental import pallas as pl
from jax.experimental.pallas import tpu as pltpu
from jax.sharding import PartitionSpec as P

MESH = pl.DeviceIdType.MESH
HIGHEST = lax.Precision.HIGHEST
F32 = jnp.float32
BF16 = jnp.bfloat16


def dot(a, b):
    return jnp.dot(a, b, precision=HIGHEST, preferred_element_type=F32)


def split(a):
    high = a.astype(BF16)
    return high, (a - high.astype(F32)).astype(BF16)


def dot_split(a_high, a_low, b_high, b_low):
    rows = a_high.shape[0]
    both = jnp.dot(
        jnp.concatenate([a_high, a_low], axis=0), b_high, preferred_element_type=F32
    )
    cross = jnp.dot(a_high, b_low, preferred_element_type=F32)
    return both[:rows] + (both[rows:] + cross)


def kernel(
    n_x, n_z, parts,
    slab_ref, panel_ref, pivots_ref, pivot_row_ref, inv_lower_ref, inv_upper_ref,
    out_ref,
    raw, lower, stage, landed, inv_lower, inv_upper, inv_split,
    picked, partner_part, chip_sum, from_x, total, halves, upper,
    load_sem, link_send, link_recv, product_send, product_recv,
    pick_send, pick_recv, x_send, x_recv, half_send, half_recv, raw_peer, peer_send, peer_recv,
):
    slab = out_ref
    prow = lax.axis_index("prow")
    pcol = lax.axis_index("pcol")
    x, core = prow // 2, prow % 2
    z, y = pcol // 2, pcol % 2
    rows = panel_ref.shape[0]
    nb = panel_ref.shape[1]
    piece = rows // parts
    row_count, columns = slab_ref.shape
    half = columns // 2
    first_row = prow * row_count
    partner = {"prow": x * 2 + 1 - core}
    peer = {"pcol": z * 2 + 1 - y}
    left = {"pcol": (z - 1) * 2 + y}
    right = {"pcol": (z + 1) * 2 + y}
    has_left, has_right = z > 0, z < n_z - 1

    loads = [
        pltpu.make_async_copy(slab_ref, slab, load_sem.at[0]),
        pltpu.make_async_copy(panel_ref, raw.at[z], load_sem.at[1]),
        pltpu.make_async_copy(inv_upper_ref, inv_upper, load_sem.at[2]),
        pltpu.make_async_copy(inv_lower_ref, inv_lower, load_sem.at[3]),
    ]
    for load in loads:
        load.start()

    barrier = pltpu.get_barrier_semaphore()
    fixed = [partner, peer] + [
        {"prow": lax.rem(x + o, n_x) * 2 + core} for o in range(1, n_x)
    ]
    for device in fixed:
        pl.semaphore_signal(barrier, inc=1, device_id=device, device_id_type=MESH)
    for exists, device in ((has_left, left), (has_right, right)):
        @pl.when(exists)
        def _():
            pl.semaphore_signal(barrier, inc=1, device_id=device, device_id_type=MESH)
    n_peers = len(fixed) + has_left.astype(jnp.int32) + has_right.astype(jnp.int32)
    pl.semaphore_wait(barrier, n_peers)

    def slot(direction, step, g):
        return (direction * (n_z - 1) + step) * parts + g

    def send(direction, step, g):
        block = z - step if direction == 0 else z + step
        span = pl.ds(g * piece, piece)
        source = panel_ref.at[span] if isinstance(step, int) else raw.at[block, span]
        return pltpu.make_async_remote_copy(
            src_ref=source,
            dst_ref=raw.at[block, span],
            send_sem=link_send.at[slot(direction, step, g)],
            recv_sem=link_recv.at[slot(direction, step, g)],
            device_id=right if direction == 0 else left,
            device_id_type=MESH,
        )

    def sends(direction, step):
        if direction == 0:
            return has_right & (z - step >= 0)
        return has_left & (z + step < n_z)

    def receives(direction, step):
        if direction == 0:
            return z - 1 - step >= 0
        return z + 1 + step < n_z

    def arrived(direction, step, g):
        block = z - 1 - step if direction == 0 else z + 1 + step
        span = pl.ds(g * piece, piece)
        pltpu.make_async_remote_copy(
            src_ref=raw.at[block, span],
            dst_ref=raw.at[block, span],
            send_sem=link_send.at[slot(direction, step, g)],
            recv_sem=link_recv.at[slot(direction, step, g)],
            device_id=left if direction == 0 else right,
            device_id_type=MESH,
        ).wait_recv()
        return block

    for g in range(parts):
        for direction in (0, 1):
            @pl.when(sends(direction, 0))
            def _():
                send(direction, 0, g).start()

    def peer_copy(g):
        span = pl.ds(g * piece, piece)
        return pltpu.make_async_remote_copy(
            src_ref=panel_ref.at[span], dst_ref=raw_peer.at[span],
            send_sem=peer_send.at[g], recv_sem=peer_recv.at[g],
            device_id=peer, device_id_type=MESH,
        )

    for g in range(parts):
        peer_copy(g).start()

    loads[0].wait()

    def pick(k, carry):
        local = pivots_ref[k] - first_row
        inside = (local >= 0) & (local < row_count)
        row = slab[pl.ds(jnp.where(inside, local, 0), 1), :]
        row = jnp.where(inside, row, 0.0)
        picked[0, pl.ds(k, 1), :] = row[:, :half]
        picked[1, pl.ds(k, 1), :] = row[:, half:]
        return carry

    lax.fori_loop(0, nb, pick, 0, unroll=8)

    def remote(source, target, send_sem, recv_sem, device):
        return pltpu.make_async_remote_copy(
            src_ref=source, dst_ref=target, send_sem=send_sem, recv_sem=recv_sem,
            device_id=device, device_id_type=MESH,
        )

    pick_copy = remote(picked.at[1 - core], partner_part, pick_send, pick_recv, partner)
    pick_copy.start()

    def pivot_hits(block, side, g):
        row = first_row + (block * 2 + side) * rows + g * piece
        ids = row + lax.broadcasted_iota(jnp.int32, (piece, nb), 0)
        hits = jnp.where(ids == pivot_row_ref[...], 1.0, 0.0)
        return hits, jnp.max(hits, axis=1, keepdims=True) > 0.0

    def make_lower(block, g):
        span = pl.ds(g * piece, piece)
        high, low = split(raw[block, span, :])
        solved = dot_split(high, low, inv_split[0], inv_split[1])
        hits, is_pivot = pivot_hits(block, y, g)
        high, low = split(jnp.where(is_pivot, -hits, solved))
        lower[0, block, span, :] = high
        lower[1, block, span, :] = low

    pick_copy.wait()
    chip_sum[...] = picked[core] + partner_part[...]
    x_copies = []
    for o in range(1, n_x):
        device = {"prow": lax.rem(x + o, n_x) * 2 + core}
        copy = remote(chip_sum, from_x.at[o - 1], x_send.at[o - 1], x_recv.at[o - 1], device)
        copy.start()
        x_copies.append(copy)

    loads[1].wait()
    loads[2].wait()
    loads[3].wait()
    inv_split[0], inv_split[1] = split(inv_upper[...])
    lax.fori_loop(0, parts, lambda g, c: (make_lower(z, g), c)[1], 0)

    for copy in x_copies:
        copy.wait()
    summed = chip_sum[...]
    for o in range(1, n_x):
        summed = summed + from_x[o - 1]
    total[...] = summed
    halves[core] = dot(inv_lower[...], total[...])
    to_peer = remote(
        halves.at[core], halves.at[2 + core], half_send.at[0], half_recv.at[0], peer
    )
    to_partner = remote(
        halves.at[core], halves.at[core], half_send.at[1], half_recv.at[1], partner
    )
    to_peer.start()
    to_partner.start()

    def pass_on(step, g):
        for direction in (0, 1):
            @pl.when(receives(direction, step))
            def _():
                arrived(direction, step, g)

            @pl.when(receives(direction, step) & sends(direction, step + 1))
            def _():
                send(direction, step + 1, g).start()

    def blocks_of(stage_index):
        step = stage_index - 1
        return (
            (receives(0, step), z - 1 - step),
            (receives(1, step), z + 1 + step),
        )

    def first_stage(g, carry):
        pass_on(jnp.int32(0), g)
        for exists, block in blocks_of(1):
            @pl.when(exists)
            def _():
                make_lower(block, g)
        return carry

    lax.fori_loop(0, parts, first_stage, 0)

    to_partner.wait()
    to_peer.wait()
    onward = remote(
        halves.at[2 + core], halves.at[2 + core], half_send.at[2], half_recv.at[2], partner
    )
    onward.start()
    for i in (0, 1):
        upper[0, :, i * half:(i + 1) * half], upper[1, :, i * half:(i + 1) * half] = (
            split(halves[i])
        )
    onward.wait()
    for i in (2, 3):
        upper[0, :, i * half:(i + 1) * half], upper[1, :, i * half:(i + 1) * half] = (
            split(halves[i])
        )

    def product_copy(block, g):
        span = pl.ds(g * piece, piece)
        index = block * parts + g
        return remote(
            stage.at[block, span], landed.at[block, span],
            product_send.at[index], product_recv.at[index], peer,
        )

    def finish(block, side, g, product, is_pivot):
        start = (block * 2 + side) * rows + g * piece
        span = pl.ds(pl.multiple_of(start, 8), piece)
        slab[span, :] = jnp.where(is_pivot, 0.0, slab[span, :]) - product

    def multiply(block, g):
        span = pl.ds(g * piece, piece)
        products = dot_split(
            lower[0, block, span, :], lower[1, block, span, :], upper[0], upper[1]
        )
        stage[block, span, :] = products[:, columns:]
        product_copy(block, g).start()
        _, is_pivot = pivot_hits(block, y, g)
        finish(block, y, g, products[:, :columns], is_pivot)

    def take(block, g):
        product_copy(block, g).wait_recv()
        _, is_pivot = pivot_hits(block, 1 - y, g)
        span = pl.ds(g * piece, piece)
        finish(block, 1 - y, g, landed[block, span, :], is_pivot)

    def multiply_own(g):
        span = pl.ds(g * piece, piece)
        _, is_pivot = pivot_hits(z, y, g)
        product = dot_split(
            lower[0, z, span, :], lower[1, z, span, :],
            upper[0, :, :columns], upper[1, :, :columns],
        )
        finish(z, y, g, product, is_pivot)

    def take_peer(g):
        peer_copy(g).wait_recv()
        high, low = split(raw_peer[pl.ds(g * piece, piece), :])
        solved = dot_split(high, low, inv_split[0], inv_split[1])
        hits, is_pivot = pivot_hits(z, 1 - y, g)
        high, low = split(jnp.where(is_pivot, -hits, solved))
        product = dot_split(high, low, upper[0, :, :columns], upper[1, :, :columns])
        finish(z, 1 - y, g, product, is_pivot)

    def second_stage(g, carry):
        for exists, block in blocks_of(1):
            @pl.when(exists)
            def _():
                multiply(block, g)
        return carry

    lax.fori_loop(0, parts, second_stage, 0)
    lax.fori_loop(0, parts, lambda g, c: (multiply_own(g), c)[1], 0)

    def late_stage(i, carry):
        stage_index, g = 2 + i // parts, i % parts
        pass_on(stage_index - 1, g)
        for exists, block in blocks_of(stage_index):
            @pl.when(exists)
            def _():
                make_lower(block, g)
                multiply(block, g)

        @pl.when(stage_index == 2)
        def _():
            take_peer(g)

        for exists, block in blocks_of(stage_index - 2):
            @pl.when(exists & (stage_index > 2))
            def _():
                take(block, g)
        return carry

    lax.fori_loop(0, (n_z - 2) * parts, late_stage, 0)

    def last_stage(i, carry):
        stage_index, g = n_z - 2 + i // parts, i % parts

        if n_z == 2:
            @pl.when(stage_index == 0)
            def _():
                take_peer(g)

        for exists, block in blocks_of(stage_index):
            @pl.when(exists & (stage_index > 0))
            def _():
                take(block, g)
        return carry

    lax.fori_loop(0, 2 * parts, last_stage, 0)

    def settle(i, carry):
        block, g = i // parts, i % parts

        @pl.when(block != z)
        def _():
            product_copy(block, g).wait_send()

        @pl.when(block == z)
        def _():
            peer_copy(g).wait_send()
        return carry

    lax.fori_loop(0, n_z * parts, settle, 0)

    def settle_links(i, carry):
        step, g = i // parts, i % parts
        for direction in (0, 1):
            @pl.when(sends(direction, step))
            def _():
                send(direction, step, g).wait_send()
        return carry

    lax.fori_loop(0, (n_z - 1) * parts, settle_links, 0)


def solution(mesh):
    n_prow, n_pcol = mesh.shape["prow"], mesh.shape["pcol"]
    n_x, n_z, parts = n_prow // 2, n_pcol // 2, 4

    def local(slab, panel, pivots, inv_lower, inv_upper):
        (row_count, columns), (rows, nb) = slab.shape, panel.shape
        half = columns // 2
        links = 2 * (n_z - 1) * parts
        hbm = pl.BlockSpec(memory_space=pltpu.HBM)
        dma = pltpu.SemaphoreType.DMA
        flops = 2 * row_count * nb * (nb + columns)
        return pl.pallas_call(
            functools.partial(kernel, n_x, n_z, parts),
            out_shape=pltpu.VMEM(slab.shape, slab.dtype),
            in_specs=[
                hbm,
                hbm,
                pl.BlockSpec(memory_space=pltpu.SMEM),
                pl.BlockSpec(memory_space=pltpu.VMEM),
                hbm,
                hbm,
            ],
            out_specs=pl.BlockSpec(memory_space=pltpu.VMEM),
            scratch_shapes=[
                pltpu.VMEM((n_z, rows, nb), F32),
                pltpu.VMEM((2, n_z, rows, nb), BF16),
                pltpu.VMEM((n_z, rows, columns), F32),
                pltpu.VMEM((n_z, rows, columns), F32),
                pltpu.VMEM((nb, nb), F32),
                pltpu.VMEM((nb, nb), F32),
                pltpu.VMEM((2, nb, nb), BF16),
                pltpu.VMEM((2, nb, half), F32),
                pltpu.VMEM((nb, half), F32),
                pltpu.VMEM((nb, half), F32),
                pltpu.VMEM((max(n_x - 1, 1), nb, half), F32),
                pltpu.VMEM((nb, half), F32),
                pltpu.VMEM((4, nb, half), F32),
                pltpu.VMEM((2, nb, 2 * columns), BF16),
                dma((4,)),
                dma((links,)),
                dma((links,)),
                dma((n_z * parts,)),
                dma((n_z * parts,)),
                dma,
                dma,
                dma((max(n_x - 1, 1),)),
                dma((max(n_x - 1, 1),)),
                dma((3,)),
                dma((3,)),
                pltpu.VMEM((rows, nb), F32),
                dma((parts,)),
                dma((parts,)),
            ],
            compiler_params=pltpu.CompilerParams(
                collective_id=0, has_side_effects=True, vmem_limit_bytes=32 * 2**20
            ),
            cost_estimate=pl.CostEstimate(
                flops=flops, bytes_accessed=8 * slab.size, transcendentals=0
            ),
        )(
            *(pltpu.with_memory_space_constraint(a, pltpu.HBM) for a in (slab, panel)),
            pivots,
            pivots.reshape(1, nb),
            *(pltpu.with_memory_space_constraint(a, pltpu.HBM) for a in (inv_lower, inv_upper)),
        )

    return jax.shard_map(
        local,
        mesh=mesh,
        in_specs=(P("prow", "pcol"), P(("prow", "pcol"), None), P(), P(), P()),
        out_specs=P("prow", "pcol"),
        check_vma=False,
    )
```
